32 devices in a mesh: groups: 2 (over x), seq: 16 (over z, y, core).
Axes of the slice: x: 2, y: 2, z: 4, core: 2. Of those that a mesh axis runs over, the one named last changes fastest.
Arguments:
- candidates: bfloat16 [32, 256, 256], P('groups', 'seq'), parts along dimension 0, may hold values from -110 to 110
- codes: int32 [32, 2048, 256], P('groups', 'seq'), parts along dimension 0, may hold values from -2147483648 to 2147483647
- scale_index: int32 [32, 8192], P('groups', 'seq'), parts along dimension 0, may hold values from 0 to 255
- lengths: int32 [32], P('groups'), parts along dimension 0, may hold values from 128 to 8192, as said below
- scale_table: float32 [256], replicated, may hold values from 0.004 to 0.04
- query_weight: bfloat16 [256, 256], replicated, may hold values from -0.375 to 0.375
- key_weight: bfloat16 [256, 256], replicated, may hold values from -0.375 to 0.375
- value_weight: bfloat16 [256, 256], replicated, may hold values from -0.375 to 0.375
- out_weight: bfloat16 [256, 256], replicated, may hold values from -0.375 to 0.375
- norm_gain: float32 [256], replicated, may hold values from 0.1 to 1.9
- hidden_weight: bfloat16 [256, 512], replicated, may hold values from -0.375 to 0.375
- hidden_bias: float32 [512], replicated, may hold values from -4 to 4
- score_weight: bfloat16 [512], replicated, may hold values from -0.25 to 0.25
Outputs:
- interest: bfloat16 [32, 256, 256], P('groups', 'seq'), parts along dimension 0
- logits: float32 [32, 256], P('groups', 'seq'), parts along dimension 0
The draws below stay inside these ranges and needn't reach their ends.
There are 2 independent parts, one for each index of `groups`. The reference program is written for one: setup_inputs(seed, part) draws one part's arguments, and reference() takes and returns one part's arrays. A program takes and returns all parts, laid end to end along the dimension named above; an argument that names none is the same for every part. Nothing has to cross between parts.
Inputs may be any that keep to these rules, and one draw needn't show every extreme that they name: `lengths`: each user's history length is a multiple of 128; in every draw some user's length is 8192.
All inputs are finite; a program needn't handle non-finite values.
Results may differ from the reference program's by a relative error of at most 0.02.
The reference program's roundings to bfloat16 on the way count: a program that leaves them out, or rounds other values in their place, can miss the bound.
Values may be sent and summed in bfloat16 or wider, within the bound.
A program may use at most 128 MiB of HBM per device.

```python
import math
import jax
import jax.numpy as jnp
from jax import lax

WIDTH = 256
HEADS = 4
RANK_HIDDEN = 512
LEVELS = 256
LGRAIN = 128
USERS = 16
CAND = 256
HIST = 8192


def draw_candidates(key, part):
    base_key = jax.random.fold_in(jax.random.fold_in(key, 5), 0)
    scale_key = jax.random.fold_in(jax.random.fold_in(key, 5), 1)
    class_key = jax.random.fold_in(jax.random.fold_in(key, 5), 2)
    weak_key = jax.random.fold_in(jax.random.fold_in(key, 5), 4)
    shape = (USERS, CAND, WIDTH)
    row_class = jax.random.uniform(class_key, (USERS, CAND, 1), jnp.float32)
    weak = jnp.exp(jax.random.uniform(weak_key, (USERS, CAND, 1), jnp.float32, math.log(0.05), math.log(0.3)))
    medium = jnp.exp(jax.random.uniform(scale_key, (USERS, CAND, 1), jnp.float32, math.log(1.5), math.log(7.0)))
    values = jnp.clip(jax.random.normal(base_key, shape, jnp.float32), -6.0, 6.0)
    row_scales = jnp.where(row_class < 0.5, weak, medium)
    return (values * row_scales).astype(jnp.bfloat16)


def draw_codes(key, part):
    tilt_key, regime_key, sign_key, high_key, low_key, full_key = jax.random.split(jax.random.fold_in(key, 7), 6)
    word_count = HIST // 4
    block_count = HIST // LGRAIN
    shape = (USERS, word_count, WIDTH)
    tilt = jax.random.randint(tilt_key, (USERS, 1), 0, 4)
    regime = jax.random.randint(regime_key, (USERS, block_count), 0, 3)
    regime = jnp.where(tilt == 0, 0, regime)
    per_word = jnp.repeat(regime, LGRAIN // 4, axis=1)[:, :, None]
    packed = jnp.zeros(shape, jnp.int32)
    for k in range(4):
        signs = jax.random.randint(jax.random.fold_in(sign_key, k), shape, 0, 2) * 2 - 1
        high = signs * jax.random.randint(jax.random.fold_in(high_key, k), shape, 100, 128)
        low = jax.random.randint(jax.random.fold_in(low_key, k), shape, -12, 13)
        full = jax.random.randint(jax.random.fold_in(full_key, k), shape, -128, 128)
        byte_value = jnp.where(per_word == 2, high, jnp.where(per_word == 1, full, low)).astype(jnp.int32)
        packed = jnp.bitwise_or(packed, jnp.left_shift(jnp.bitwise_and(byte_value, 255), 8 * k))
    return packed


def draw_lengths(key, part):
    first_key, second_key = jax.random.split(jax.random.fold_in(key, 11))
    granules = jax.random.randint(first_key, (USERS,), 1, HIST // LGRAIN + 1)
    longest = jax.random.randint(second_key, (), 0, USERS)
    granules = jnp.where(jnp.arange(USERS, dtype=jnp.int32) == longest, HIST // LGRAIN, granules)
    return (granules * LGRAIN).astype(jnp.int32)


def set_ends(values, stream_key, low, top_value):
    dims = values.shape
    index_at = [jax.random.randint(jax.random.fold_in(stream_key, axis), (), 0, dims[axis]) for axis in range(len(dims))]
    values = values.at[tuple(index_at)].set(low)
    longest = dims.index(max(dims))
    index_at[longest] = (index_at[longest] + 1) % dims[longest]
    return values.at[tuple(index_at)].set(top_value)


def centred(stream_key, extent, width, limit, kind=jnp.bfloat16):
    values = jax.random.normal(stream_key, extent, jnp.float32) * width
    return jnp.minimum(jnp.maximum(values, -limit), limit).astype(kind)


def setup_inputs(seed: int = 0, part: int = 0) -> dict:
    arg_keys = jax.random.split(jax.random.key(seed), 14)
    part_keys = jax.random.split(jax.random.fold_in(arg_keys[13], part), 14)
    candidates = draw_candidates(jax.random.fold_in(jax.random.fold_in(arg_keys[13], part), 71), part)
    codes = draw_codes(jax.random.fold_in(jax.random.fold_in(arg_keys[13], part), 71), part)
    scale_index = set_ends(jax.random.randint(part_keys[2], (USERS, HIST), 0, LEVELS), jax.random.fold_in(part_keys[2], 1), 0, LEVELS - 1).astype(jnp.int32)
    lengths = draw_lengths(jax.random.fold_in(jax.random.fold_in(arg_keys[13], part), 71), part)
    scale_table = jnp.clip(jnp.exp(jax.random.uniform(arg_keys[4], (LEVELS,), jnp.float32, math.log(0.004), math.log(0.04))), 0.004, 0.04)
    query_weight = centred(arg_keys[5], (WIDTH, WIDTH), WIDTH ** -0.5, 0.375)
    key_weight = centred(arg_keys[6], (WIDTH, WIDTH), WIDTH ** -0.5, 0.375)
    value_weight = centred(arg_keys[7], (WIDTH, WIDTH), WIDTH ** -0.5, 0.375)
    out_weight = centred(arg_keys[8], (WIDTH, WIDTH), WIDTH ** -0.5, 0.375)
    norm_gain = jnp.clip(1.0 + 0.18 * jax.random.normal(arg_keys[9], (WIDTH,), jnp.float32), 0.1, 1.9)
    hidden_weight = centred(arg_keys[10], (WIDTH, RANK_HIDDEN), WIDTH ** -0.5, 0.375)
    hidden_bias = centred(arg_keys[11], (RANK_HIDDEN,), 1.0, 4.0, jnp.float32)
    score_weight = centred(arg_keys[12], (RANK_HIDDEN,), RANK_HIDDEN ** -0.5, 0.25)
    return dict(candidates=candidates, codes=codes, scale_index=scale_index, lengths=lengths, scale_table=scale_table, query_weight=query_weight, key_weight=key_weight, value_weight=value_weight, out_weight=out_weight, norm_gain=norm_gain, hidden_weight=hidden_weight, hidden_bias=hidden_bias, score_weight=score_weight)


NEG_FILL = -1e+30

def unpack_codes(words):
    byte_rows = [jnp.right_shift(jnp.left_shift(words, 24 - 8 * k), 24) for k in range(4)]
    stacked = jnp.stack(byte_rows, axis=1)
    return stacked.reshape(words.shape[0] * 4, words.shape[1])

def reference(candidates, codes, scale_index, lengths, scale_table, query_weight, key_weight, value_weight, out_weight, norm_gain, hidden_weight, hidden_bias, score_weight):
    head_size = WIDTH // HEADS
    inv_root = 1.0 / math.sqrt(head_size)
    positions = jnp.arange(HIST, dtype=jnp.int32)

    def one_user(user_item):
        cand_rows, word_rows, index_rows, user_length = user_item
        code_rows = unpack_codes(word_rows)
        history = (code_rows.astype(jnp.float32) * scale_table[index_rows][:, None]).astype(jnp.bfloat16)
        all_keys = jnp.dot(history, key_weight, preferred_element_type=jnp.float32).astype(jnp.bfloat16)
        all_values = jnp.dot(history, value_weight, preferred_element_type=jnp.float32).astype(jnp.bfloat16)
        queries = jnp.dot(cand_rows, query_weight, preferred_element_type=jnp.float32).astype(jnp.bfloat16)
        live_mask = positions < user_length

        def one_head(head_index):
            start = (head_index * head_size).astype(jnp.int32)
            query_head = lax.dynamic_slice_in_dim(queries, start, head_size, 1)
            key_head = lax.dynamic_slice_in_dim(all_keys, start, head_size, 1)
            value_head = lax.dynamic_slice_in_dim(all_values, start, head_size, 1)
            scores = jnp.dot(query_head, key_head.T, preferred_element_type=jnp.float32) * inv_root
            scores = jnp.where(live_mask[None, :], scores, NEG_FILL)
            peak_rows = lax.optimization_barrier(jnp.max(scores, axis=1, keepdims=True))
            weights = jnp.where(live_mask[None, :], jnp.exp(scores - peak_rows), 0.0)
            totals = lax.optimization_barrier(jnp.sum(weights, axis=1, keepdims=True))
            numerators = jnp.dot(weights.astype(jnp.bfloat16), value_head, preferred_element_type=jnp.float32)
            return numerators / totals
        head_outs = lax.map(one_head, jnp.arange(HEADS, dtype=jnp.int32))
        attended = jnp.transpose(head_outs, (1, 0, 2)).reshape(CAND, WIDTH).astype(jnp.bfloat16)
        interest = jnp.dot(attended, out_weight, preferred_element_type=jnp.float32).astype(jnp.bfloat16)
        floats = interest.astype(jnp.float32)
        normed = (floats * lax.rsqrt(lax.optimization_barrier(jnp.mean(floats * floats, axis=1, keepdims=True)) + 1e-06) * norm_gain).astype(jnp.bfloat16)
        hidden = jax.nn.silu(jnp.dot(normed, hidden_weight, preferred_element_type=jnp.float32) + hidden_bias).astype(jnp.bfloat16)
        logits = jnp.dot(hidden, score_weight, preferred_element_type=jnp.float32)
        return (interest, logits)
    interest, logits = lax.map(one_user, (candidates, codes, scale_index, lengths))
    return (interest, logits)
```

```python
import functools
import math

import jax
import jax.numpy as jnp
from jax import lax
from jax.experimental import pallas as pl
from jax.experimental.pallas import tpu as pltpu
from jax.sharding import PartitionSpec as P

HEADS = 4
MESH = pl.DeviceIdType.MESH
DEAD = -1e30
NT = (((1,), (1,)), ((), ()))


def mm(a, b, dims=(((1,), (0,)), ((), ()))):
    return lax.dot_general(a, b, dims, preferred_element_type=jnp.float32)


def kernel(
    n,
    chunk,
    lengths,
    cand,
    codes_hbm,
    index,
    table,
    wq,
    wk,
    wv,
    wo,
    gain,
    wh,
    bias,
    ws,
    interest_out,
    logits_out,
    codes,
    scales,
    wkv,
    qown,
    qall,
    kvown,
    kvsend,
    kvrecv,
    nsend,
    stats,
    nrecv,
    srecv,
    attended,
    code_sem,
    q_ssem,
    q_rsem,
    kv_ssem,
    kv_rsem,
    n_ssem,
    n_rsem,
    s_ssem,
    s_rsem,
):
    users, cl, width = cand.shape
    words = codes.shape[1]
    hist = 4 * words
    half = width // 2
    hs = width // HEADS
    rows = n * cl
    me = lax.axis_index("seq")
    core = lax.rem(me, 2)
    partner = me + 1 - 2 * core
    fetch = pltpu.make_async_copy(codes_hbm, codes, code_sem)
    fetch.start()

    def peer(i):
        return lax.rem(me + (2 * n - i - 1), n)

    barrier = pltpu.get_barrier_semaphore()
    for i in range(n - 1):
        pl.semaphore_signal(barrier, inc=1, device_id={"seq": peer(i)}, device_id_type=MESH)

    queries = (mm(cand[...].reshape(users * cl, width), wq[...])).astype(jnp.bfloat16)
    queries = (queries.astype(jnp.float32) * (1.0 / math.sqrt(hs))).astype(jnp.bfloat16)
    q3 = queries.reshape(users, cl, width)
    qown[0] = q3[:, :, :half]
    qown[1] = q3[:, :, half:]
    mine_q = jnp.where(core == 0, q3[:, :, :half].astype(jnp.float32), q3[:, :, half:].astype(jnp.float32))
    qall[:, n - 1] = mine_q.astype(jnp.bfloat16)

    pl.semaphore_wait(barrier, n - 1)

    def remote(src, dst, ssem, rsem, dev):
        return pltpu.make_async_remote_copy(
            src_ref=src, dst_ref=dst, send_sem=ssem, recv_sem=rsem,
            device_id={"seq": dev}, device_id_type=MESH,
        )

    for c in range(users // chunk):
        part = pl.ds(c * chunk, chunk)
        for i in range(n - 1):
            dev = peer(n - 2 - i)
            remote(
                qown.at[lax.rem(dev, 2), part], qall.at[part, i],
                q_ssem, q_rsem.at[c], dev,
            ).start()

    first = core == 0

    def pick(w, a):
        lo, hi = w[:, :half].astype(jnp.float32), w[:, half:].astype(jnp.float32)
        return jnp.where(a, lo, hi).astype(jnp.bfloat16)

    other = core == 1
    wkv[:, 0:half] = pick(wk[...], first)
    wkv[:, half:2 * half] = pick(wv[...], first)
    wkv[:, 2 * half:3 * half] = pick(wk[...], other)
    wkv[:, 3 * half:] = pick(wv[...], other)

    ids = index[...].reshape(users * 8, index.shape[2])
    low = lax.bitwise_and(ids, 127)
    found = jnp.zeros(ids.shape, jnp.float32)
    for g in range(table.shape[0]):
        line = jnp.broadcast_to(table[g:g + 1, :], (ids.shape[0], 128))
        got = jnp.take_along_axis(line, low, axis=1, mode="promise_in_bounds")
        found = jnp.where(lax.shift_right_logical(ids, 7) == g, got, found)
    scales[...] = found.reshape(scales.shape)
    stats[...] = jnp.zeros_like(stats)
    fetch.wait()

    lane = lax.broadcasted_iota(jnp.int32, (1, half), 1)
    head0 = lane < hs

    def project(u):
        word = codes[u]
        cols = jnp.transpose(scales[u])
        parts = []
        for k in range(4):
            code = lax.shift_right_arithmetic(lax.shift_left(word, jnp.int32(24 - 8 * k)), jnp.int32(24))
            parts.append((code.astype(jnp.float32) * cols[:, k:k + 1]).astype(jnp.bfloat16))
        history = jnp.concatenate(parts, axis=0)
        kvown[u] = mm(history, wkv[:, :width]).astype(jnp.bfloat16)
        kvsend[u] = mm(history, wkv[:, width:]).astype(jnp.bfloat16)
        remote(kvsend.at[u], kvrecv.at[u], kv_ssem.at[u], kv_rsem.at[u], partner).start()

    spot = lax.broadcasted_iota(jnp.int32, (1, hist), 1)
    spot = 4 * lax.rem(spot, words) + lax.div(spot, words)

    def attend(u):
        remote(kvsend.at[u], kvrecv.at[u], kv_ssem.at[u], kv_rsem.at[u], partner).wait()
        q = qall[u].reshape(rows, half)
        length = lengths[u]
        biases = [
            jnp.where(spot + dev * hist < length, 0.0, DEAD) for dev in (me, partner)
        ]
        outs, peaks = [], []
        for h in range(2):
            on = head0 if h == 0 else jnp.logical_not(head0)
            qh = jnp.where(on, q, jnp.zeros_like(q))
            s = [
                mm(qh, kv[u][:, :half], NT) + b
                for kv, b in zip((kvown, kvrecv), biases)
            ]
            peak = jnp.max(jnp.maximum(s[0], s[1]), axis=1, keepdims=True)
            acc = None
            for kv, x in zip((kvown, kvrecv), s):
                v = kv[u][:, half:]
                v = jnp.where(on, v, jnp.ones_like(v))
                o = mm(jnp.exp(x - peak).astype(jnp.bfloat16), v)
                acc = o if acc is None else acc + o
            outs.append(acc)
            peaks.append(peak)
        nsend[u] = jnp.where(head0, outs[0], outs[1]).astype(jnp.bfloat16).reshape(n, cl, half)
        values = (peaks[0], peaks[1], outs[0][:, hs:hs + 1], outs[1][:, 0:1])
        st = stats[...].reshape(rows, 128)
        wide = lax.broadcasted_iota(jnp.int32, (1, 128), 1)
        for r in range(4):
            st = jnp.where(wide == 4 * u + r, values[r], st)
        stats[...] = st.reshape(stats.shape)
        for i in range(n - 1):
            remote(nsend.at[u, i], nrecv.at[i, u], n_ssem, n_rsem, peer(i)).start()
        nrecv[n - 1, u] = nsend[u, n - 1]

    project(0)

    def group(c, carry):
        landed = qall.at[pl.ds(c * chunk, chunk), pl.ds(0, n - 1)]
        remote(landed, landed, q_ssem, q_rsem.at[c], partner).wait_recv()

        def body(k, carry):
            u = c * chunk + k

            @pl.when(u + 1 < users)
            def _():
                project(u + 1)

            attend(u)
            return carry

        return lax.fori_loop(0, chunk, body, carry)

    lax.fori_loop(0, users // chunk, group, 0)

    for i in range(n - 1):
        remote(stats.at[i], srecv.at[i], s_ssem, s_rsem, peer(i)).start()
    srecv[n - 1] = stats[n - 1]
    qdone = qall.at[:, pl.ds(0, n - 1)]
    remote(qdone, qdone, q_ssem, q_rsem.at[0], partner).wait_send()
    sdone = srecv.at[pl.ds(0, n - 1)]
    remote(sdone, sdone, s_ssem, s_rsem, partner).wait()
    ndone = nrecv.at[pl.ds(0, n - 1)]
    remote(ndone, ndone, n_ssem, n_rsem, partner).wait()

    shares = [None] * n
    for parity in range(2):
        slots = range(parity, n, 2)
        top = functools.reduce(jnp.maximum, [srecv[i] for i in slots])
        factors = [jnp.exp(srecv[i] - top) for i in slots]
        sums = [f * pltpu.roll(srecv[i], 126, axis=1) for f, i in zip(factors, slots)]
        total = functools.reduce(jnp.add, sums)
        for f, i in zip(factors, slots):
            shares[i] = f / total
    share = jnp.concatenate(shares, axis=0)
    stats[...] = share.reshape(stats.shape)

    def merge(u, carry):
        turned = pltpu.roll(stats[...].reshape(rows, 128), lax.rem(128 - 4 * u, 128), axis=1)
        scale = jnp.where(head0, turned[:, 0:1], turned[:, 1:2])
        part = nrecv[:, u].astype(jnp.float32) * scale.reshape(n, cl, half)
        same = functools.reduce(jnp.add, [part[i] for i in range(1, n, 2)])
        cross = functools.reduce(jnp.add, [part[i] for i in range(0, n, 2)])
        attended[u, :, :half] = jnp.where(first, same, cross).astype(jnp.bfloat16)
        attended[u, :, half:] = jnp.where(first, cross, same).astype(jnp.bfloat16)
        return carry

    lax.fori_loop(0, users, merge, 0)

    interest = mm(attended[...].reshape(users * cl, width), wo[...]).astype(jnp.bfloat16)
    interest_out[...] = interest.reshape(users, cl, width)
    floats = interest.astype(jnp.float32)
    spread = jnp.mean(floats * floats, axis=1, keepdims=True)
    normed = (floats * lax.rsqrt(spread + 1e-06) * gain[...]).astype(jnp.bfloat16)
    v = mm(normed, wh[...]) + bias[...]
    hidden = (v / (1.0 + jnp.exp(-v))).astype(jnp.bfloat16)
    logits_out[...] = mm(jnp.broadcast_to(ws[...], (16, ws.shape[1])), hidden, NT)[0:1]


def on_device(
    n,
    candidates,
    codes,
    scale_index,
    lengths,
    scale_table,
    query_weight,
    key_weight,
    value_weight,
    out_weight,
    norm_gain,
    hidden_weight,
    hidden_bias,
    score_weight,
):
    users, cl, width = candidates.shape
    words = codes.shape[1]
    half = width // 2
    chunk = math.gcd(users, 4)
    index = jnp.transpose(scale_index.reshape(users, words, 4), (0, 2, 1))
    index = jnp.pad(index, ((0, 0), (0, 4), (0, 0)))
    vmem = pl.BlockSpec(memory_space=pltpu.VMEM)
    interest, logits = pl.pallas_call(
        functools.partial(kernel, n, chunk),
        out_shape=(
            jax.ShapeDtypeStruct((users, cl, width), jnp.bfloat16),
            jax.ShapeDtypeStruct((1, users * cl), jnp.float32),
        ),
        in_specs=[pl.BlockSpec(memory_space=pltpu.SMEM), vmem, pl.BlockSpec(memory_space=pl.ANY)] + [vmem] * 10,
        out_specs=(vmem, vmem),
        scratch_shapes=[
            pltpu.VMEM((users, words, width), jnp.int32),
            pltpu.VMEM((users, 8, words), jnp.float32),
            pltpu.VMEM((width, 2 * width), jnp.bfloat16),
            pltpu.VMEM((2, users, cl, half), jnp.bfloat16),
            pltpu.VMEM((users, n, cl, half), jnp.bfloat16),
            pltpu.VMEM((users, 4 * words, width), jnp.bfloat16),
            pltpu.VMEM((users, 4 * words, width), jnp.bfloat16),
            pltpu.VMEM((users, 4 * words, width), jnp.bfloat16),
            pltpu.VMEM((users, n, cl, half), jnp.bfloat16),
            pltpu.VMEM((n, cl, 128), jnp.float32),
            pltpu.VMEM((n, users, cl, half), jnp.bfloat16),
            pltpu.VMEM((n, cl, 128), jnp.float32),
            pltpu.VMEM((users, cl, width), jnp.bfloat16),
            pltpu.SemaphoreType.DMA,
            pltpu.SemaphoreType.DMA,
            pltpu.SemaphoreType.DMA((users // chunk,)),
            pltpu.SemaphoreType.DMA((users,)),
            pltpu.SemaphoreType.DMA((users,)),
            pltpu.SemaphoreType.DMA,
            pltpu.SemaphoreType.DMA,
            pltpu.SemaphoreType.DMA,
            pltpu.SemaphoreType.DMA,
        ],
        compiler_params=pltpu.CompilerParams(
            collective_id=0, has_side_effects=True, vmem_limit_bytes=60 * 1024 * 1024
        ),
    )(
        lengths,
        candidates,
        codes,
        index,
        scale_table.reshape(-1, 128),
        query_weight,
        key_weight,
        value_weight,
        out_weight,
        norm_gain.reshape(1, -1),
        hidden_weight,
        hidden_bias.reshape(1, -1),
        score_weight.reshape(1, -1),
    )
    return interest, logits.reshape(users, cl)


def solution(mesh):
    placed = (
        P("groups", "seq", None),
        P("groups", "seq", None),
        P("groups", "seq"),
        P("groups"),
    ) + (P(),) * 9
    return jax.shard_map(
        functools.partial(on_device, mesh.shape["seq"]),
        mesh=mesh,
        in_specs=placed,
        out_specs=(P("groups", "seq", None), P("groups", "seq")),
        check_vma=False,
    )
```

```python
import functools
import math

import jax
import jax.numpy as jnp
from jax import lax
from jax.experimental import pallas as pl
from jax.experimental.pallas import tpu as pltpu
from jax.sharding import PartitionSpec as P

HEADS = 4
MESH = pl.DeviceIdType.MESH
DEAD = -1e30
NT = (((1,), (1,)), ((), ()))


def mm(a, b, dims=(((1,), (0,)), ((), ()))):
    return lax.dot_general(a, b, dims, preferred_element_type=jnp.float32)


def kernel(
    n,
    chunk,
    lengths,
    cand,
    codes_hbm,
    index,
    table,
    wq,
    wk,
    wv,
    wo,
    gain,
    wh,
    bias,
    ws,
    interest_out,
    logits_out,
    codes,
    scales,
    wkv,
    qown,
    qall,
    kvown,
    kvsend,
    kvrecv,
    nsend,
    stats,
    nrecv,
    srecv,
    attended,
    code_sem,
    q_ssem,
    q_rsem,
    f_ssem,
    f_rsem,
    kv_ssem,
    kv_rsem,
    n_ssem,
    n_rsem,
    s_ssem,
    s_rsem,
):
    users, cl, width = cand.shape
    words = codes.shape[1]
    hist = 4 * words
    half = width // 2
    hs = width // HEADS
    rows = n * cl
    me = lax.axis_index("seq")
    core = lax.rem(me, 2)
    partner = me + 1 - 2 * core
    fetch = pltpu.make_async_copy(codes_hbm, codes, code_sem)
    fetch.start()

    near = n // 2

    def peer(i):
        there = me
        for bit in range(n.bit_length() - 1):
            place = 0 if bit == 0 else bit - 1 if bit > 1 else n.bit_length() - 2
            if (i >> place) & 1:
                there = there + (1 << bit) * (1 - 2 * lax.rem(lax.div(me, 1 << bit), 2))
        return there

    barrier = pltpu.get_barrier_semaphore()
    for i in range(1, n):
        pl.semaphore_signal(barrier, inc=1, device_id={"seq": peer(i)}, device_id_type=MESH)

    queries = (mm(cand[...].reshape(users * cl, width), wq[...])).astype(jnp.bfloat16)
    queries = (queries.astype(jnp.float32) * (1.0 / math.sqrt(hs))).astype(jnp.bfloat16)
    q3 = queries.reshape(users, cl, width)
    qown[0] = q3[:, :, :half]
    qown[1] = q3[:, :, half:]
    mine_q = jnp.where(core == 0, q3[:, :, :half].astype(jnp.float32), q3[:, :, half:].astype(jnp.float32))
    qall[:, 0] = mine_q.astype(jnp.bfloat16)

    pl.semaphore_wait(barrier, n - 1)

    def remote(src, dst, ssem, rsem, dev):
        return pltpu.make_async_remote_copy(
            src_ref=src, dst_ref=dst, send_sem=ssem, recv_sem=rsem,
            device_id={"seq": dev}, device_id_type=MESH,
        )

    for c in range(users // chunk):
        part = pl.ds(c * chunk, chunk)
        for i in range(1, near):
            dev = peer(i)
            remote(
                qown.at[lax.rem(dev, 2), part], qall.at[part, i], q_ssem, q_rsem.at[c], dev
            ).start()
        remote(qall.at[part, 0], qall.at[part, near], f_ssem, f_rsem.at[c], peer(near)).start()

    first = core == 0

    def pick(w, a):
        lo, hi = w[:, :half].astype(jnp.float32), w[:, half:].astype(jnp.float32)
        return jnp.where(a, lo, hi).astype(jnp.bfloat16)

    other = core == 1
    wkv[:, 0:half] = pick(wk[...], first)
    wkv[:, half:2 * half] = pick(wv[...], first)
    wkv[:, 2 * half:3 * half] = pick(wk[...], other)
    wkv[:, 3 * half:] = pick(wv[...], other)

    place = lax.broadcasted_iota(jnp.int32, (users, 128), 1)

    def lookup(line, at):
        return jnp.take_along_axis(line, at, axis=1, mode="promise_in_bounds")

    for block in range(words // 128):
        for k in range(4):
            ids = jnp.zeros((users, 128), jnp.int32)
            for j in range(4):
                start = 512 * block + 128 * j
                got = lookup(index[:, start:start + 128], 4 * lax.rem(place, 32) + k)
                ids = jnp.where(lax.div(place, 32) == j, got, ids)
            found = jnp.zeros((users, 128), jnp.float32)
            for g in range(table.shape[0]):
                line = jnp.broadcast_to(table[g:g + 1, :], (users, 128))
                got = lookup(line, lax.bitwise_and(ids, 127))
                found = jnp.where(lax.shift_right_logical(ids, 7) == g, got, found)
            scales[:, k, 128 * block:128 * block + 128] = found
    stats[...] = jnp.zeros_like(stats)
    fetch.wait()

    lane = lax.broadcasted_iota(jnp.int32, (1, half), 1)
    head0 = lane < hs

    def project(u):
        word = codes[u]
        cols = jnp.transpose(scales[u])
        parts = []
        for k in range(4):
            code = lax.shift_right_arithmetic(lax.shift_left(word, jnp.int32(24 - 8 * k)), jnp.int32(24))
            parts.append((code.astype(jnp.float32) * cols[:, k:k + 1]).astype(jnp.bfloat16))
        history = jnp.concatenate(parts, axis=0)
        kvown[u] = mm(history, wkv[:, :width]).astype(jnp.bfloat16)
        kvsend[u] = mm(history, wkv[:, width:]).astype(jnp.bfloat16)
        remote(kvsend.at[u], kvrecv.at[u], kv_ssem.at[u], kv_rsem.at[u], partner).start()

    spot = lax.broadcasted_iota(jnp.int32, (1, hist), 1)
    spot = 4 * lax.rem(spot, words) + lax.div(spot, words)

    def attend(u):
        remote(kvsend.at[u], kvrecv.at[u], kv_ssem.at[u], kv_rsem.at[u], partner).wait()
        q = qall[u].reshape(rows, half)
        length = lengths[u]
        biases = [
            jnp.where(spot + dev * hist < length, 0.0, DEAD) for dev in (me, partner)
        ]
        outs, peaks = [], []
        for h in range(2):
            on = head0 if h == 0 else jnp.logical_not(head0)
            qh = jnp.where(on, q, jnp.zeros_like(q))
            s = [
                mm(qh, kv[u][:, :half], NT) + b
                for kv, b in zip((kvown, kvrecv), biases)
            ]
            peak = jnp.max(jnp.maximum(s[0], s[1]), axis=1, keepdims=True)
            acc = None
            for kv, x in zip((kvown, kvrecv), s):
                v = kv[u][:, half:]
                v = jnp.where(on, v, jnp.ones_like(v))
                o = mm(jnp.exp(x - peak).astype(jnp.bfloat16), v)
                acc = o if acc is None else acc + o
            outs.append(acc)
            peaks.append(peak)
        nsend[u] = jnp.where(head0, outs[0], outs[1]).astype(jnp.bfloat16).reshape(n, cl, half)
        values = (peaks[0], peaks[1], outs[0][:, hs:hs + 1], outs[1][:, 0:1])
        st = stats[...].reshape(rows, 128)
        wide = lax.broadcasted_iota(jnp.int32, (1, 128), 1)
        for r in range(4):
            st = jnp.where(wide == 4 * u + r, values[r], st)
        stats[...] = st.reshape(stats.shape)
        for i in range(1, n):
            remote(nsend.at[u, i], nrecv.at[i, u], n_ssem, n_rsem, peer(i)).start()
        nrecv[0, u] = nsend[u, 0]

    def forward(c):
        landed = qall.at[pl.ds(c * chunk, chunk), pl.ds(1, near - 1)]
        remote(landed, landed, q_ssem, q_rsem.at[c], partner).wait_recv()
        target = qall.at[pl.ds(c * chunk, chunk), pl.ds(near + 1, near - 1)]
        remote(landed, target, f_ssem, f_rsem.at[c], peer(near)).start()

    groups = users // chunk
    project(0)
    forward(0)

    def group(c, carry):
        @pl.when(c + 1 < groups)
        def _():
            forward(c + 1)

        landed = qall.at[pl.ds(c * chunk, chunk), pl.ds(near, near)]
        remote(landed, landed, f_ssem, f_rsem.at[c], partner).wait_recv()

        def body(k, carry):
            u = c * chunk + k

            @pl.when(u + 1 < users)
            def _():
                project(u + 1)

            attend(u)
            return carry

        return lax.fori_loop(0, chunk, body, carry)

    lax.fori_loop(0, groups, group, 0)

    for i in range(1, n):
        remote(stats.at[i], srecv.at[i], s_ssem, s_rsem, peer(i)).start()
    srecv[0] = stats[0]
    qdone = qall.at[:, pl.ds(1, near - 1)]
    remote(qdone, qdone, q_ssem, q_rsem.at[0], partner).wait_send()
    fdone = qall.at[:, pl.ds(near, near)]
    remote(fdone, fdone, f_ssem, f_rsem.at[0], partner).wait_send()
    sdone = srecv.at[pl.ds(1, n - 1)]
    remote(sdone, sdone, s_ssem, s_rsem, partner).wait()
    ndone = nrecv.at[pl.ds(1, n - 1)]
    remote(ndone, ndone, n_ssem, n_rsem, partner).wait()

    shares = [None] * n
    for parity in range(2):
        slots = range(parity, n, 2)
        top = functools.reduce(jnp.maximum, [srecv[i] for i in slots])
        factors = [jnp.exp(srecv[i] - top) for i in slots]
        sums = [f * pltpu.roll(srecv[i], 126, axis=1) for f, i in zip(factors, slots)]
        total = functools.reduce(jnp.add, sums)
        for f, i in zip(factors, slots):
            shares[i] = f / total
    share = jnp.concatenate(shares, axis=0)
    wide = lax.broadcasted_iota(jnp.int32, (1, 128), 1)
    used = jnp.logical_and(lax.rem(wide, 4) < 2, wide < 4 * users)
    share = jnp.where(used, share, 0.0)
    high = share.astype(jnp.bfloat16)
    low = (share - high.astype(jnp.float32)).astype(jnp.bfloat16)
    share = jnp.concatenate([high, low], axis=1)
    source = lax.rem(lax.broadcasted_iota(jnp.int32, (256, half), 0), 128)
    target = lax.div(lax.broadcasted_iota(jnp.int32, (256, half), 1), hs)

    def merge(u, carry):
        spread = jnp.where(source == 4 * u + target, 1.0, 0.0).astype(jnp.bfloat16)
        scale = mm(share, spread)
        part = nrecv[:, u].astype(jnp.float32) * scale.reshape(n, cl, half)
        same = functools.reduce(jnp.add, [part[i] for i in range(0, n, 2)])
        cross = functools.reduce(jnp.add, [part[i] for i in range(1, n, 2)])
        attended[u, :, :half] = jnp.where(first, same, cross).astype(jnp.bfloat16)
        attended[u, :, half:] = jnp.where(first, cross, same).astype(jnp.bfloat16)
        return carry

    lax.fori_loop(0, users, merge, 0)

    interest = mm(attended[...].reshape(users * cl, width), wo[...]).astype(jnp.bfloat16)
    interest_out[...] = interest.reshape(users, cl, width)
    floats = interest.astype(jnp.float32)
    spread = jnp.mean(floats * floats, axis=1, keepdims=True)
    normed = (floats * lax.rsqrt(spread + 1e-06) * gain[...]).astype(jnp.bfloat16)
    v = mm(normed, wh[...]) + bias[...]
    hidden = (v / (1.0 + jnp.exp(-v))).astype(jnp.bfloat16)
    line = mm(jnp.broadcast_to(ws[...].astype(jnp.float32).reshape(1, -1), (16, ws.shape[0])).astype(jnp.bfloat16), hidden, NT)[0:1]
    row = lax.broadcasted_iota(jnp.int32, (users, users * cl), 0)
    column = lax.broadcasted_iota(jnp.int32, (users, users * cl), 1)
    spread = jnp.where(lax.div(column, cl) == row, line, 0.0)
    chosen = lax.rem(lax.broadcasted_iota(jnp.int32, (users * cl, cl), 0), cl)
    chosen = (chosen == lax.broadcasted_iota(jnp.int32, (users * cl, cl), 1)).astype(jnp.float32)
    logits_out[...] = lax.dot_general(
        spread, chosen, (((1,), (0,)), ((), ())),
        precision=lax.Precision.HIGHEST, preferred_element_type=jnp.float32,
    )


def on_device(
    n,
    candidates,
    codes,
    scale_index,
    lengths,
    scale_table,
    query_weight,
    key_weight,
    value_weight,
    out_weight,
    norm_gain,
    hidden_weight,
    hidden_bias,
    score_weight,
):
    users, cl, width = candidates.shape
    words = codes.shape[1]
    half = width // 2
    chunk = math.gcd(users, 2)
    vmem = pl.BlockSpec(memory_space=pltpu.VMEM)
    return pl.pallas_call(
        functools.partial(kernel, n, chunk),
        out_shape=(
            jax.ShapeDtypeStruct((users, cl, width), jnp.bfloat16),
            jax.ShapeDtypeStruct((users, cl), jnp.float32),
        ),
        in_specs=[pl.BlockSpec(memory_space=pltpu.SMEM), vmem, pl.BlockSpec(memory_space=pl.ANY)] + [vmem] * 10,
        out_specs=(vmem, vmem),
        scratch_shapes=[
            pltpu.VMEM((users, words, width), jnp.int32),
            pltpu.VMEM((users, 8, words), jnp.float32),
            pltpu.VMEM((width, 2 * width), jnp.bfloat16),
            pltpu.VMEM((2, users, cl, half), jnp.bfloat16),
            pltpu.VMEM((users, n, cl, half), jnp.bfloat16),
            pltpu.VMEM((users, 4 * words, width), jnp.bfloat16),
            pltpu.VMEM((users, 4 * words, width), jnp.bfloat16),
            pltpu.VMEM((users, 4 * words, width), jnp.bfloat16),
            pltpu.VMEM((users, n, cl, half), jnp.bfloat16),
            pltpu.VMEM((n, cl, 128), jnp.float32),
            pltpu.VMEM((n, users, cl, half), jnp.bfloat16),
            pltpu.VMEM((n, cl, 128), jnp.float32),
            pltpu.VMEM((users, cl, width), jnp.bfloat16),
            pltpu.SemaphoreType.DMA,
            pltpu.SemaphoreType.DMA,
            pltpu.SemaphoreType.DMA((users // chunk,)),
            pltpu.SemaphoreType.DMA,
            pltpu.SemaphoreType.DMA((users // chunk,)),
            pltpu.SemaphoreType.DMA((users,)),
            pltpu.SemaphoreType.DMA((users,)),
            pltpu.SemaphoreType.DMA,
            pltpu.SemaphoreType.DMA,
            pltpu.SemaphoreType.DMA,
            pltpu.SemaphoreType.DMA,
        ],
        compiler_params=pltpu.CompilerParams(
            collective_id=0, has_side_effects=True, vmem_limit_bytes=60 * 1024 * 1024
        ),
    )(
        lengths,
        candidates,
        codes,
        scale_index,
        scale_table.reshape(-1, 128),
        query_weight,
        key_weight,
        value_weight,
        out_weight,
        norm_gain.reshape(1, -1),
        hidden_weight,
        hidden_bias.reshape(1, -1),
        score_weight,
    )


def solution(mesh):
    placed = (
        P("groups", "seq", None),
        P("groups", "seq", None),
        P("groups", "seq"),
        P("groups"),
    ) + (P(),) * 9
    return jax.shard_map(
        functools.partial(on_device, mesh.shape["seq"]),
        mesh=mesh,
        in_specs=placed,
        out_specs=(P("groups", "seq", None), P("groups", "seq")),
        check_vma=False,
    )
```
